16 devices in a mesh: dp: 16 (over z, y, x, core).
Axes of the slice: x: 2, y: 2, z: 2, core: 2. Of those that a mesh axis runs over, the one named last changes fastest.
Arguments:
- token_ids: int32 [32, 384], P('dp')
- target_ids: int32 [32, 384], P('dp')
- st_wte: float32 [3, 40478, 768], P(None, None, 'dp')
- st_wpe: float32 [3, 514, 768], P(None, None, 'dp')
- st_qkv: float32 [3, 2, 768, 3, 12, 64], P(None, None, 'dp')
- st_proj: float32 [3, 2, 12, 64, 768], P(None, None, None, None, 'dp')
- st_up: float32 [3, 2, 768, 3072], P(None, None, 'dp')
- st_down: float32 [3, 2, 3072, 768], P(None, None, 'dp')
- st_vec: float32 [3, 2, 9984], P(None, None, 'dp')
- st_lnf: float32 [3, 2, 768], P(None, None, 'dp')
Outputs:
- output 1: float32 [], replicated
- output 2: float32 [3, 40478, 768], P(None, None, 'dp')
- output 3: float32 [3, 514, 768], P(None, None, 'dp')
- output 4: float32 [3, 2, 768, 3, 12, 64], P(None, None, 'dp')
- output 5: float32 [3, 2, 12, 64, 768], P(None, None, None, None, 'dp')
- output 6: float32 [3, 2, 768, 3072], P(None, None, 'dp')
- output 7: float32 [3, 2, 3072, 768], P(None, None, 'dp')
- output 8: float32 [3, 2, 9984], P(None, None, 'dp')
- output 9: float32 [3, 2, 768], P(None, None, 'dp')
All inputs are finite; a program needn't handle non-finite values.
Results may differ from the reference program's by a relative error of at most 0.00221679.
Values are sent between devices in bfloat16 or wider.
A program may use at most 1 GiB of HBM per device.

```python
import jax
import jax.numpy as jnp
from jax import lax

NUM_DEVICES = 16
BATCH_DEV = 2
SEQ_LEN = 384
D_MODEL = 768
NUM_HEADS = 12
HEAD_DIM = 64
FF_DIM = 3072
VOCAB_SIZE = 40478
MAX_POS = 512
NUM_LAYERS = 2
ADAM_STEP = 10
HOT_IDS = 16

TOTAL_ROWS = NUM_DEVICES * BATCH_DEV
POS_ROWS = MAX_POS + 2
VEC_LEN = 9 * D_MODEL + FF_DIM
INV_TOKENS = 1.0 / (TOTAL_ROWS * SEQ_LEN)
SCORE_SCALE = HEAD_DIM ** -0.5
NORM_EPS = 1e-5
LEARN_RATE = 3e-3
BETA_ONE = 0.9
BETA_TWO = 0.95
ADAM_EPS = 1e-8
WEIGHT_DECAY = 0.1
CLIP_NORM = 1.0
MOM_SCALE = 2e-6
DECAYS = (WEIGHT_DECAY,) * 6 + (0.0, 0.0)


def draw_tokens(base_key):
    k_ids, k_wide, k_hot, k_pick, k_flip = jax.random.split(base_key, 5)
    tok_grid = (TOTAL_ROWS, SEQ_LEN)
    token_ids = jax.random.randint(k_ids, tok_grid, 0, VOCAB_SIZE, jnp.int32)
    token_ids = token_ids.at[0, 0].set(VOCAB_SIZE - 1).at[0, 1].set(0)
    hot_table = jax.random.randint(k_hot, (HOT_IDS,), 0, VOCAB_SIZE, jnp.int32)
    hot_pick = hot_table[jax.random.randint(k_pick, tok_grid, 0, HOT_IDS, jnp.int32)]
    wide_pick = jax.random.randint(k_wide, tok_grid, 0, VOCAB_SIZE, jnp.int32)
    coin_flip = jax.random.randint(k_flip, tok_grid, 0, 2, jnp.int32)
    target_ids = jnp.where(coin_flip == 1, hot_pick, wide_pick)
    target_ids = target_ids.at[0, 0].set(VOCAB_SIZE - 1).at[0, 1].set(0)
    return token_ids, target_ids


def draw_state(base_key, dims, center, scale):
    k_par, k_mom, k_sec = jax.random.split(base_key, 3)
    master = center + scale * jax.random.normal(k_par, dims, jnp.float32)
    moment = MOM_SCALE * jax.random.normal(k_mom, dims, jnp.float32)
    second = (MOM_SCALE * jax.random.uniform(k_sec, dims, jnp.float32, 0.5, 1.5)) ** 2
    return jnp.stack([master, moment, second])


def setup_inputs(seed: int = 0) -> dict:
    key_list = jax.random.split(jax.random.key(seed), 9)
    token_ids, target_ids = draw_tokens(key_list[0])
    d_scale = D_MODEL ** -0.5
    vec_center = jnp.concatenate([jnp.zeros((5 * D_MODEL + FF_DIM,), jnp.float32), jnp.ones((D_MODEL,), jnp.float32), jnp.zeros((D_MODEL,), jnp.float32), jnp.ones((D_MODEL,), jnp.float32), jnp.zeros((D_MODEL,), jnp.float32)])
    lnf_center = jnp.array([[1.0], [0.0]], jnp.float32)
    lnf_scale = jnp.array([[0.2], [1.0]], jnp.float32)
    return dict(
        token_ids=token_ids,
        target_ids=target_ids,
        st_wte=draw_state(key_list[1], (VOCAB_SIZE, D_MODEL), 0.0, d_scale),
        st_wpe=draw_state(key_list[2], (POS_ROWS, D_MODEL), 0.0, d_scale),
        st_qkv=draw_state(key_list[3], (NUM_LAYERS, D_MODEL, 3, NUM_HEADS, HEAD_DIM), 0.0, d_scale),
        st_proj=draw_state(key_list[4], (NUM_LAYERS, NUM_HEADS, HEAD_DIM, D_MODEL), 0.0, d_scale),
        st_up=draw_state(key_list[5], (NUM_LAYERS, D_MODEL, FF_DIM), 0.0, d_scale),
        st_down=draw_state(key_list[6], (NUM_LAYERS, FF_DIM, D_MODEL), 0.0, FF_DIM ** -0.5),
        st_vec=draw_state(key_list[7], (NUM_LAYERS, VEC_LEN), vec_center, 0.2),
        st_lnf=draw_state(key_list[8], (2, D_MODEL), lnf_center, lnf_scale),
    )


def layer_norm(residual, gain, bias):
    mean_val = jnp.mean(residual, axis=-1, keepdims=True)
    centered = residual - mean_val
    variance = jnp.mean(centered * centered, axis=-1, keepdims=True)
    return centered * lax.rsqrt(variance + NORM_EPS) * gain.astype(jnp.float32) + bias.astype(jnp.float32)


def block(residual, qkv_w, proj_w, up_w, down_w, layer_vec):
    seq_len = residual.shape[0]
    offset = 4 * D_MODEL + FF_DIM
    ln_par = layer_vec[offset + D_MODEL:].reshape(4, D_MODEL)
    normed_in = layer_norm(residual, ln_par[0], ln_par[1]).astype(jnp.bfloat16)
    qkv_all = jnp.dot(normed_in, qkv_w.reshape(D_MODEL, 3 * D_MODEL), preferred_element_type=jnp.float32) + layer_vec[:3 * D_MODEL].astype(jnp.float32)
    qkv_all = qkv_all.astype(jnp.bfloat16).reshape(seq_len, 3, NUM_HEADS, HEAD_DIM).astype(jnp.float32)
    scores = jnp.einsum('qhk,shk->hqs', qkv_all[:, 0], qkv_all[:, 1]) * SCORE_SCALE
    causal = jnp.arange(seq_len)[:, None] >= jnp.arange(seq_len)[None, :]
    scores = jnp.where(causal[None], scores, -1e30)
    attn_prob = jax.nn.softmax(scores, axis=-1).astype(jnp.bfloat16).astype(jnp.float32)
    mixed = jnp.einsum('hqs,shk->qhk', attn_prob, qkv_all[:, 2]).astype(jnp.bfloat16)
    residual = residual + jnp.dot(mixed.reshape(seq_len, D_MODEL), proj_w.reshape(D_MODEL, D_MODEL), preferred_element_type=jnp.float32) + layer_vec[3 * D_MODEL:4 * D_MODEL].astype(jnp.float32)
    normed_mid = layer_norm(residual, ln_par[2], ln_par[3]).astype(jnp.bfloat16)
    hidden = jax.nn.relu(jnp.dot(normed_mid, up_w, preferred_element_type=jnp.float32) + layer_vec[4 * D_MODEL:offset].astype(jnp.float32)).astype(jnp.bfloat16)
    return residual + jnp.dot(hidden, down_w, preferred_element_type=jnp.float32) + layer_vec[offset:offset + D_MODEL].astype(jnp.float32)


def sequence_loss(masters, row_ids, row_tgt):
    wte_c, wpe_c, qkv_w, proj_w, up_w, down_w, vec_all, lnf_c = [w.astype(jnp.bfloat16) for w in masters]
    residual = masters[0][row_ids].astype(jnp.bfloat16).astype(jnp.float32) + wpe_c[2:2 + SEQ_LEN].astype(jnp.float32)
    for layer in range(NUM_LAYERS):
        residual = block(residual, qkv_w[layer], proj_w[layer], up_w[layer], down_w[layer], vec_all[layer])
    normed = layer_norm(residual, lnf_c[0], lnf_c[1]).astype(jnp.bfloat16)
    logits = jnp.dot(normed, wte_c.T, preferred_element_type=jnp.float32)
    picked = jnp.take_along_axis(logits, row_tgt[:, None], axis=-1)[:, 0]
    return jnp.sum(jax.nn.logsumexp(logits, axis=-1) - picked) * INV_TOKENS


def adam_update(state, grad, decay):
    moment = BETA_ONE * state[1] + (1.0 - BETA_ONE) * grad
    second = BETA_TWO * state[2] + (1.0 - BETA_TWO) * grad * grad
    m_hat = moment / (1.0 - BETA_ONE ** ADAM_STEP)
    v_hat = second / (1.0 - BETA_TWO ** ADAM_STEP)
    master = state[0] * (1.0 - LEARN_RATE * decay) - LEARN_RATE * m_hat / (jnp.sqrt(v_hat) + ADAM_EPS)
    return jnp.stack([master, moment, second])


def reference(token_ids, target_ids, st_wte, st_wpe, st_qkv, st_proj, st_up, st_down, st_vec, st_lnf):
    states = (st_wte, st_wpe, st_qkv, st_proj, st_up, st_down, st_vec, st_lnf)
    masters = tuple(state[0] for state in states)

    def row_step(carry, row):
        grad_acc, loss_acc = carry
        row_loss, row_grad = jax.value_and_grad(sequence_loss)(masters, row[0], row[1])
        return (jax.tree.map(jnp.add, grad_acc, row_grad), loss_acc + row_loss), None

    init_carry = (tuple(jnp.zeros_like(w) for w in masters), jnp.zeros((), jnp.float32))
    (grads, loss), _ = lax.scan(row_step, init_carry, (token_ids, target_ids))
    grad_norm = jnp.sqrt(sum(jnp.sum(g * g) for g in grads))
    clip_coef = jnp.minimum(1.0, CLIP_NORM / (grad_norm + 1e-6))
    new_wte, new_wpe, new_qkv, new_proj, new_up, new_down, new_vec, new_lnf = [adam_update(state, g * clip_coef, decay) for state, g, decay in zip(states, grads, DECAYS)]
    return (loss, new_wte, new_wpe, new_qkv, new_proj, new_up, new_down, new_vec, new_lnf)
```

```python
import functools

import jax
import jax.numpy as jnp
from jax import lax
from jax.experimental import pallas as pl
from jax.experimental.pallas import tpu as pltpu
from jax.sharding import PartitionSpec as P

NORM_EPS = 1e-5
LEARN_RATE = 3e-3
BETA_ONE = 0.9
BETA_TWO = 0.95
ADAM_EPS = 1e-8
WEIGHT_DECAY = 0.1
CLIP_NORM = 1.0
ADAM_STEP = 10
DECAYS = (WEIGHT_DECAY,) * 6 + (0.0, 0.0)
LANES = 128
TOKEN_TILE = 512
VOCAB_TILE = 512
VMEM_BYTES = 60 * 1024 * 1024


def layer_norm(residual, gain, bias):
    mean_val = jnp.mean(residual, axis=-1, keepdims=True)
    centered = residual - mean_val
    variance = jnp.mean(centered * centered, axis=-1, keepdims=True)
    return centered * lax.rsqrt(variance + NORM_EPS) * gain.astype(jnp.float32) + bias.astype(jnp.float32)


def attention_half(residual, qkv_w, proj_t, layer_vec, num_heads, ff_dim):
    batch, seq_len, d_model = residual.shape
    head_dim = d_model // num_heads
    offset = 4 * d_model + ff_dim
    ln_par = layer_vec[offset + d_model:].reshape(4, d_model)
    normed_in = layer_norm(residual, ln_par[0], ln_par[1]).astype(jnp.bfloat16)
    qkv_all = jnp.einsum('bsd,tde->tbse', normed_in, qkv_w, preferred_element_type=jnp.float32)
    qkv_all = (qkv_all + layer_vec[:3 * d_model].astype(jnp.float32).reshape(3, 1, 1, d_model)).astype(jnp.bfloat16)
    qkv_all = qkv_all.reshape(3, batch, seq_len, num_heads, head_dim)
    scores = jnp.einsum('bqhk,bshk->bhqs', qkv_all[0], qkv_all[1], preferred_element_type=jnp.float32) * head_dim ** -0.5
    rows_iota = lax.broadcasted_iota(jnp.int32, (seq_len, seq_len), 0)
    cols_iota = lax.broadcasted_iota(jnp.int32, (seq_len, seq_len), 1)
    scores = jnp.where(rows_iota >= cols_iota, scores, -1e30)
    attn_prob = jax.nn.softmax(scores, axis=-1).astype(jnp.bfloat16)
    mixed = jnp.einsum('bhqs,bshk->bqhk', attn_prob, qkv_all[2], preferred_element_type=jnp.float32).astype(jnp.bfloat16)
    mixed = mixed.reshape(batch, seq_len, d_model)
    return residual + jnp.einsum('bsl,el->bse', mixed, proj_t, preferred_element_type=jnp.float32) + layer_vec[3 * d_model:4 * d_model].astype(jnp.float32)


def feed_half(residual, up_w, down_w, layer_vec):
    d_model, ff_dim = up_w.shape
    offset = 4 * d_model + ff_dim
    ln_par = layer_vec[offset + d_model:].reshape(4, d_model)
    normed_mid = layer_norm(residual, ln_par[2], ln_par[3]).astype(jnp.bfloat16)
    hidden = jax.nn.relu(jnp.einsum('bsd,df->bsf', normed_mid, up_w, preferred_element_type=jnp.float32) + layer_vec[4 * d_model:offset].astype(jnp.float32)).astype(jnp.bfloat16)
    return residual + jnp.einsum('bsf,fd->bsd', hidden, down_w, preferred_element_type=jnp.float32) + layer_vec[offset:offset + d_model].astype(jnp.float32)


def final_norm(residual, lnf_c):
    return layer_norm(residual, lnf_c[0], lnf_c[1]).astype(jnp.bfloat16)


def lookup_kernel(ids_ref, table_ref, out_ref):
    def step(i, carry):
        base = pl.multiple_of(i * 8, 8)
        rows = [table_ref[pl.ds(ids_ref[base + u], 1), :] for u in range(8)]
        out_ref[pl.ds(base, 8), :] = jnp.concatenate(rows, axis=0)
        return carry

    lax.fori_loop(0, out_ref.shape[0] // 8, step, 0)


def lookup_rows(ids, table):
    count = ids.shape[0]
    return pl.pallas_call(
        lookup_kernel,
        out_shape=jax.ShapeDtypeStruct((count, LANES), jnp.float32),
        in_specs=[pl.BlockSpec(memory_space=pltpu.SMEM), pl.BlockSpec(memory_space=pltpu.VMEM)],
        out_specs=pl.BlockSpec(memory_space=pltpu.VMEM),
        compiler_params=pltpu.CompilerParams(vmem_limit_bytes=VMEM_BYTES),
        cost_estimate=pl.CostEstimate(flops=10 ** 10, bytes_accessed=count * 2 * LANES * 4 + table.size * 4, transcendentals=0),
    )(ids, table)


def accumulate_kernel(ids_ref, rows_ref, acc_ref):
    def clear(i, carry):
        acc_ref[pl.ds(pl.multiple_of(i * 512, 512), 512), :] = jnp.zeros((512, LANES), jnp.float32)
        return carry

    lax.fori_loop(0, acc_ref.shape[0] // 512, clear, 0)

    def step(i, carry):
        base = pl.multiple_of(i * 8, 8)
        rows = rows_ref[pl.ds(base, 8), :]
        for u in range(8):
            idx = ids_ref[base + u]
            acc_ref[pl.ds(idx, 1), :] = acc_ref[pl.ds(idx, 1), :] + rows[u:u + 1, :]
        return carry

    lax.fori_loop(0, rows_ref.shape[0] // 8, step, 0)


def accumulate_rows(ids, rows, num_rows):
    return pl.pallas_call(
        accumulate_kernel,
        out_shape=jax.ShapeDtypeStruct((num_rows, LANES), jnp.float32),
        in_specs=[pl.BlockSpec(memory_space=pltpu.SMEM), pl.BlockSpec(memory_space=pltpu.VMEM)],
        out_specs=pl.BlockSpec(memory_space=pltpu.VMEM),
        compiler_params=pltpu.CompilerParams(vmem_limit_bytes=VMEM_BYTES),
        cost_estimate=pl.CostEstimate(flops=10 ** 10, bytes_accessed=rows.size * 4 + num_rows * LANES * 4, transcendentals=0),
    )(ids, rows)


def head_forward_kernel(h_ref, head_ref, mask_ref, u_ref, lse_ref, logit_ref):
    h_tile = h_ref[...]
    slice_len = head_ref.shape[1]
    top = jnp.full((h_tile.shape[0], 1), -jnp.inf, jnp.float32)
    for start in range(0, slice_len, VOCAB_TILE):
        cols = slice(start, start + VOCAB_TILE)
        logits = jnp.dot(h_tile, head_ref[:, cols], preferred_element_type=jnp.float32) + mask_ref[:, cols]
        logit_ref[:, cols] = logits
        top = jnp.maximum(top, jnp.max(logits, axis=-1, keepdims=True))
    total = jnp.zeros_like(top)
    for start in range(0, slice_len, VOCAB_TILE):
        cols = slice(start, start + VOCAB_TILE)
        exp_shift = jnp.exp(logit_ref[:, cols] - top)
        total = total + jnp.sum(exp_shift, axis=-1, keepdims=True)
        part = lax.dot_general(exp_shift.astype(jnp.bfloat16), head_ref[:, cols], (((1,), (1,)), ((), ())), preferred_element_type=jnp.float32)
        if start == 0:
            u_ref[...] = part
        else:
            u_ref[...] += part
    u_ref[...] = u_ref[...] * (1.0 / total)
    lse_ref[...] = top + jnp.log(total)


def head_forward(h_all, head_t, mask):
    tokens, d_model = h_all.shape
    slice_len = head_t.shape[1]
    return pl.pallas_call(
        head_forward_kernel,
        grid=(tokens // TOKEN_TILE,),
        out_shape=(jax.ShapeDtypeStruct((tokens, d_model), jnp.float32), jax.ShapeDtypeStruct((tokens, 1), jnp.float32)),
        in_specs=[pl.BlockSpec((TOKEN_TILE, d_model), lambda i: (i, 0)), pl.BlockSpec((d_model, slice_len), lambda i: (0, 0)), pl.BlockSpec((1, slice_len), lambda i: (0, 0))],
        out_specs=(pl.BlockSpec((TOKEN_TILE, d_model), lambda i: (i, 0)), pl.BlockSpec((TOKEN_TILE, 1), lambda i: (i, 0))),
        scratch_shapes=[pltpu.VMEM((TOKEN_TILE, slice_len), jnp.float32)],
        compiler_params=pltpu.CompilerParams(vmem_limit_bytes=VMEM_BYTES, dimension_semantics=('arbitrary',)),
        cost_estimate=pl.CostEstimate(flops=4 * tokens * d_model * slice_len, bytes_accessed=tokens * d_model * 6 + head_t.size * 2, transcendentals=tokens * slice_len),
    )(h_all, head_t, mask)


def head_grad_kernel(inv_tokens, h_ref, head_ref, mask_ref, lse_ref, tgt_ref, grad_ref, flip_ref):
    h_tile = h_ref[...]
    slice_len = head_ref.shape[1]
    flip_ref[...] = jnp.transpose(h_tile)
    lse = lse_ref[...]
    tgt = tgt_ref[...]

    @pl.when(pl.program_id(0) == 0)
    def _():
        grad_ref[...] = jnp.zeros_like(grad_ref)

    for start in range(0, slice_len, VOCAB_TILE):
        cols = slice(start, start + VOCAB_TILE)
        logits = jnp.dot(h_tile, head_ref[:, cols], preferred_element_type=jnp.float32) + mask_ref[:, cols]
        prob = jnp.exp(logits - lse) * inv_tokens
        is_target = lax.broadcasted_iota(jnp.int32, logits.shape, 1) == tgt - start
        d_logits = jnp.where(is_target, prob - inv_tokens, prob).astype(jnp.bfloat16)
        grad_ref[:, cols] += jnp.dot(flip_ref[...], d_logits, preferred_element_type=jnp.float32)


def head_grad(h_all, head_t, mask, lse, tgt, inv_tokens):
    tokens, d_model = h_all.shape
    slice_len = head_t.shape[1]
    return pl.pallas_call(
        functools.partial(head_grad_kernel, inv_tokens),
        grid=(tokens // TOKEN_TILE,),
        out_shape=jax.ShapeDtypeStruct((d_model, slice_len), jnp.float32),
        in_specs=[pl.BlockSpec((TOKEN_TILE, d_model), lambda i: (i, 0)), pl.BlockSpec((d_model, slice_len), lambda i: (0, 0)), pl.BlockSpec((1, slice_len), lambda i: (0, 0)), pl.BlockSpec((TOKEN_TILE, 1), lambda i: (i, 0)), pl.BlockSpec((TOKEN_TILE, 1), lambda i: (i, 0))],
        out_specs=pl.BlockSpec((d_model, slice_len), lambda i: (0, 0)),
        scratch_shapes=[pltpu.VMEM((d_model, TOKEN_TILE), jnp.bfloat16)],
        compiler_params=pltpu.CompilerParams(vmem_limit_bytes=VMEM_BYTES, dimension_semantics=('arbitrary',)),
        cost_estimate=pl.CostEstimate(flops=4 * tokens * d_model * slice_len, bytes_accessed=tokens * d_model * 2 + head_t.size * 6, transcendentals=tokens * slice_len),
    )(h_all, head_t, mask, lse, tgt)


def adam_update(state, grad, decay):
    moment = BETA_ONE * state[1] + (1.0 - BETA_ONE) * grad
    second = BETA_TWO * state[2] + (1.0 - BETA_TWO) * grad * grad
    m_hat = moment / (1.0 - BETA_ONE ** ADAM_STEP)
    v_hat = second / (1.0 - BETA_TWO ** ADAM_STEP)
    master = state[0] * (1.0 - LEARN_RATE * decay) - LEARN_RATE * m_hat / (jnp.sqrt(v_hat) + ADAM_EPS)
    return jnp.stack([master, moment, second])


def solution(mesh):
    n_dev = mesh.shape['dp']
    row_spec = P('dp', None)
    state_specs = (P(None, None, 'dp'), P(None, None, 'dp'), P(None, None, 'dp', None, None, None), P(None, None, None, None, 'dp'), P(None, None, 'dp', None), P(None, None, 'dp', None), P(None, None, 'dp'), P(None, None, 'dp'))

    def gather(local):
        return lax.all_gather(local, 'dp', axis=0, tiled=False)

    def scatter_sum(full):
        return lax.psum_scatter(full, 'dp', scatter_dimension=0, tiled=False)

    def swap(blocks):
        return lax.all_to_all(blocks, 'dp', split_axis=0, concat_axis=0, tiled=False)

    def train_step(token_ids, target_ids, st_wte, st_wpe, st_qkv, st_proj, st_up, st_down, st_vec, st_lnf):
        num_layers, shard = st_qkv.shape[1], st_qkv.shape[2]
        num_heads = st_qkv.shape[4]
        batch_dev, seq_len = token_ids.shape
        vocab_size = st_wte.shape[1]
        pos_rows = st_wpe.shape[1]
        d_model = shard * n_dev
        ff_shard = st_down.shape[2]
        ff_dim = ff_shard * n_dev
        ff_parts = ff_dim // d_model
        vec_shard = st_vec.shape[2]
        tok_dev = batch_dev * seq_len
        tokens = tok_dev * n_dev
        inv_tokens = 1.0 / tokens
        slice_len = -(-vocab_size // (n_dev * VOCAB_TILE)) * VOCAB_TILE
        vocab_pad = slice_len * n_dev
        me = lax.axis_index('dp')

        def pack_attn(qkv, proj):
            return [jnp.swapaxes(qkv.reshape(shard, 3, d_model), 0, 1).reshape(3 * shard, d_model), proj.reshape(d_model, shard).T]

        def pack_feed(up, down):
            return [jnp.swapaxes(up.reshape(shard, ff_parts, d_model), 0, 1).reshape(ff_parts * shard, d_model), down]

        pos_pack = st_wpe[0, 2:2 + seq_len].T.reshape(-1, d_model)
        pos_count = pos_pack.shape[0]
        small_rows = jnp.concatenate([st_vec[0], jnp.pad(st_lnf[0].reshape(1, -1), ((0, 0), (0, vec_shard - 2 * shard)))], axis=0)
        small_rows = jnp.pad(small_rows, ((0, (-(num_layers + 1 + pos_count)) % 16), (0, d_model - vec_shard)))

        def half_pack(parts):
            return jnp.concatenate([part.astype(jnp.bfloat16) for part in parts], axis=0)

        gathered_attn, gathered_feed = [], []
        for layer in range(num_layers):
            parts = pack_attn(st_qkv[0, layer], st_proj[0, layer])
            if layer == 0:
                parts = parts + [pos_pack, small_rows]
            gathered_attn.append(gather(half_pack(parts)))
            gathered_feed.append(gather(half_pack(pack_feed(st_up[0, layer], st_down[0, layer]))))

        ids_all = lax.all_gather(jnp.stack([token_ids, target_ids]), 'dp', axis=1, tiled=True).reshape(2, tokens)
        table = jnp.pad(st_wte[0], ((0, 0), (0, LANES - shard)))

        def spread_rows(rows):
            cols = rows[:, :shard].astype(jnp.bfloat16).T.reshape(shard, n_dev, tok_dev)
            return swap(jnp.swapaxes(cols, 0, 1)).reshape(d_model, tok_dev).T

        token_rows = spread_rows(lookup_rows(ids_all[0], table))

        attn_rows = 4 * shard
        first = gathered_attn[0]
        pos_c = first[:, attn_rows:attn_rows + pos_count].reshape(d_model, seq_len).T
        small_c = first[:, attn_rows + pos_count:attn_rows + pos_count + num_layers + 1, :vec_shard]
        vec_c = [small_c[:, layer].reshape(-1) for layer in range(num_layers)]
        lnf_c = jnp.swapaxes(small_c[:, num_layers, :2 * shard].reshape(n_dev, 2, shard), 0, 1).reshape(2, d_model)

        def attn_weights(block):
            qkv_w = jnp.swapaxes(block[:, :3 * shard].reshape(n_dev, 3, shard, d_model), 0, 1).reshape(3, d_model, d_model)
            return qkv_w, block[:, 3 * shard:attn_rows].reshape(d_model, d_model)

        def feed_weights(block):
            up_w = jnp.swapaxes(block[:, :ff_parts * shard].reshape(n_dev, ff_parts, shard, d_model), 1, 2).reshape(d_model, ff_dim)
            return up_w, block[:, ff_parts * shard:].reshape(ff_dim, d_model)

        residual = token_rows.astype(jnp.float32).reshape(batch_dev, seq_len, d_model) + pos_c.astype(jnp.float32)
        attn_backs, feed_backs = [], []
        for layer in range(num_layers):
            qkv_w, proj_t = attn_weights(gathered_attn[layer])
            residual, back = jax.vjp(lambda x, a, b, c: attention_half(x, a, b, c, num_heads, ff_dim), residual, qkv_w, proj_t, vec_c[layer])
            attn_backs.append(back)
            up_w, down_w = feed_weights(gathered_feed[layer])
            residual, back = jax.vjp(feed_half, residual, up_w, down_w, vec_c[layer])
            feed_backs.append(back)
        normed, norm_back = jax.vjp(final_norm, residual, lnf_c)

        head_send = jnp.pad(st_wte[0].T.astype(jnp.bfloat16), ((0, 0), (0, vocab_pad - vocab_size)))
        head_send = jnp.swapaxes(head_send.reshape(shard, n_dev, slice_len), 0, 1)
        head_t = swap(head_send).reshape(d_model, slice_len)
        vocab_pos = me * slice_len + lax.broadcasted_iota(jnp.int32, (1, slice_len), 1)
        mask = jnp.where(vocab_pos < vocab_size, 0.0, -1e30).astype(jnp.float32)
        tgt_local = (ids_all[1] - me * slice_len).reshape(n_dev, batch_dev, seq_len)

        h_alls = [gather(normed[row]).reshape(n_dev * seq_len, d_model) for row in range(batch_dev)]
        late_ids, _ = lax.optimization_barrier((ids_all[1], normed))
        target_rows = spread_rows(lookup_rows(late_ids, table)).astype(jnp.float32).reshape(batch_dev, seq_len, d_model)
        lse_alls, d_parts, loss_part = [], [], 0.0
        for row in range(batch_dev):
            u_part, lse_part = head_forward(h_alls[row], head_t, mask)
            lse_dev = lax.all_gather(lse_part.reshape(-1), 'dp', axis=0, tiled=False)
            top = jnp.max(lse_dev, axis=0)
            lse = top + jnp.log(jnp.sum(jnp.exp(lse_dev - top), axis=0))
            factor = jnp.exp(lse_part - lse[:, None]) * inv_tokens
            d_sum = scatter_sum((u_part * factor).reshape(n_dev, seq_len, d_model))
            d_parts.append(d_sum - inv_tokens * target_rows[row])
            lse_alls.append(lse[:, None])
            own = lax.dynamic_slice_in_dim(lse, me * seq_len, seq_len)
            picked = jnp.sum(normed[row].astype(jnp.float32) * target_rows[row], axis=-1)
            loss_part = loss_part + jnp.sum(own - picked) * inv_tokens
        d_normed = jnp.stack(d_parts)
        head_parts = [head_grad(h_alls[row], head_t, mask, lse_alls[row], tgt_local[:, row].reshape(-1, 1), inv_tokens) for row in range(batch_dev)]
        grad_head = functools.reduce(jnp.add, head_parts)
        grad_head = swap(grad_head.reshape(n_dev, shard, slice_len))
        grad_head = jnp.swapaxes(grad_head, 0, 1).reshape(shard, vocab_pad)[:, :vocab_size].T

        d_resid, d_lnf = norm_back(d_normed.astype(jnp.bfloat16))
        d_vec = [None] * num_layers
        qkv_g, proj_g, up_g, down_g = ([None] * num_layers for _ in range(4))
        small_g = None
        for layer in reversed(range(num_layers)):
            d_resid, d_up, d_down, d_vec_b = feed_backs[layer](d_resid)
            up_rows = jnp.swapaxes(d_up.reshape(n_dev, shard, ff_parts, d_model), 1, 2).reshape(n_dev, ff_parts * shard, d_model)
            summed = scatter_sum(jnp.concatenate([up_rows, d_down.reshape(n_dev, ff_shard, d_model)], axis=1).astype(jnp.float32))
            up_g[layer] = jnp.swapaxes(summed[:ff_parts * shard].reshape(ff_parts, shard, d_model), 0, 1).reshape(shard, ff_dim)
            down_g[layer] = summed[ff_parts * shard:]
            d_resid, d_qkv, d_proj, d_vec_a = attn_backs[layer](d_resid)
            d_vec[layer] = d_vec_a + d_vec_b
            qkv_rows = jnp.swapaxes(d_qkv.reshape(3, n_dev, shard, d_model), 0, 1).reshape(n_dev, 3 * shard, d_model)
            parts = [qkv_rows.astype(jnp.float32), d_proj.reshape(n_dev, shard, d_model).astype(jnp.float32)]
            if layer == 0:
                pos_sum = jnp.sum(d_resid, axis=0).T.reshape(n_dev, pos_count, d_model)
                rows = [vec.astype(jnp.float32).reshape(n_dev, 1, vec_shard) for vec in d_vec]
                rows.append(jnp.pad(jnp.swapaxes(d_lnf.astype(jnp.float32).reshape(2, n_dev, shard), 0, 1).reshape(n_dev, 1, 2 * shard), ((0, 0), (0, 0), (0, vec_shard - 2 * shard))))
                rows = jnp.concatenate(rows, axis=1)
                rows = jnp.pad(rows, ((0, 0), (0, (-(num_layers + 1 + pos_count)) % 8), (0, d_model - vec_shard)))
                parts = parts + [pos_sum, rows]
            summed = scatter_sum(jnp.concatenate(parts, axis=1))
            qkv_g[layer] = jnp.swapaxes(summed[:3 * shard].reshape(3, shard, d_model), 0, 1).reshape(st_qkv.shape[2:])
            proj_g[layer] = summed[3 * shard:attn_rows].T.reshape(st_proj.shape[2:])
            if layer == 0:
                pos_g = jnp.pad(summed[attn_rows:attn_rows + pos_count].reshape(shard, seq_len).T, ((2, pos_rows - 2 - seq_len), (0, 0)))
                small_g = summed[attn_rows + pos_count:attn_rows + pos_count + num_layers + 1, :vec_shard]
        vec_g = small_g[:num_layers]
        lnf_g = small_g[num_layers, :2 * shard].reshape(2, shard)

        lookup_d = swap(d_resid.reshape(tok_dev, d_model).T.reshape(n_dev, shard, tok_dev))
        lookup_d = jnp.pad(jnp.swapaxes(lookup_d, 1, 2).reshape(tokens, shard), ((0, 0), (0, LANES - shard)))
        wte_g = grad_head + accumulate_rows(ids_all[0], lookup_d, vocab_pad)[:vocab_size, :shard]

        grads = [wte_g, pos_g, jnp.stack(qkv_g), jnp.stack(proj_g), jnp.stack(up_g), jnp.stack(down_g), vec_g, lnf_g]
        local_sq = sum(jnp.sum(grad * grad) for grad in grads)
        sums = lax.psum(jnp.stack([local_sq, loss_part]), 'dp')
        clip_coef = jnp.minimum(1.0, CLIP_NORM / (jnp.sqrt(sums[0]) + 1e-6))
        states = (st_wte, st_wpe, st_qkv, st_proj, st_up, st_down, st_vec, st_lnf)
        new_states = tuple(adam_update(state, grad * clip_coef, decay) for state, grad, decay in zip(states, grads, DECAYS))
        return (sums[1],) + new_states

    return jax.shard_map(train_step, mesh=mesh, in_specs=(row_spec, row_spec) + state_specs, out_specs=(P(),) + state_specs, check_vma=False)
```

```python
import functools

import jax
import jax.numpy as jnp
from jax import lax
from jax.experimental import pallas as pl
from jax.experimental.pallas import tpu as pltpu
from jax.sharding import PartitionSpec as P

NORM_EPS = 1e-5
LEARN_RATE = 3e-3
BETA_ONE = 0.9
BETA_TWO = 0.95
ADAM_EPS = 1e-8
WEIGHT_DECAY = 0.1
CLIP_NORM = 1.0
ADAM_STEP = 10
DECAYS = (WEIGHT_DECAY,) * 6 + (0.0, 0.0)
LANES = 128
TOKEN_TILE = 512
VOCAB_TILE = 512
GRAD_TILE = 640
VMEM_BYTES = 60 * 1024 * 1024


def layer_norm(residual, gain, bias):
    mean_val = jnp.mean(residual, axis=-1, keepdims=True)
    centered = residual - mean_val
    variance = jnp.mean(centered * centered, axis=-1, keepdims=True)
    return centered * lax.rsqrt(variance + NORM_EPS) * gain.astype(jnp.float32) + bias.astype(jnp.float32)


def affine(x, weight, bias):
    return jnp.einsum('bsd,de->bse', x, weight, preferred_element_type=jnp.float32) + bias


def attention_half(residual, wq, wk, wv, proj_t, bq, bk, bv, bo, gain, shift, num_heads):
    batch, seq_len, d_model = residual.shape
    head_dim = d_model // num_heads
    normed_in = layer_norm(residual, gain, shift).astype(jnp.bfloat16)
    q, k, v = (affine(normed_in, w, b).astype(jnp.bfloat16).reshape(batch, seq_len, num_heads, head_dim) for w, b in ((wq, bq), (wk, bk), (wv, bv)))
    scores = jnp.einsum('bqhk,bshk->bhqs', q, k, preferred_element_type=jnp.float32) * head_dim ** -0.5
    rows_iota = lax.broadcasted_iota(jnp.int32, (seq_len, seq_len), 0)
    cols_iota = lax.broadcasted_iota(jnp.int32, (seq_len, seq_len), 1)
    scores = jnp.where(rows_iota >= cols_iota, scores, -1e30)
    attn_prob = jax.nn.softmax(scores, axis=-1).astype(jnp.bfloat16)
    mixed = jnp.einsum('bhqs,bshk->bqhk', attn_prob, v, preferred_element_type=jnp.float32).astype(jnp.bfloat16)
    mixed = mixed.reshape(batch, seq_len, d_model)
    return residual + jnp.einsum('bsl,el->bse', mixed, proj_t, preferred_element_type=jnp.float32) + bo


def feed_half(residual, ups, downs, b1s, b2, gain, shift):
    normed_mid = layer_norm(residual, gain, shift).astype(jnp.bfloat16)
    out = residual + b2
    for up_w, down_w, b1 in zip(ups, downs, b1s):
        hidden = jax.nn.relu(affine(normed_mid, up_w, b1)).astype(jnp.bfloat16)
        out = out + jnp.einsum('bsf,fd->bsd', hidden, down_w, preferred_element_type=jnp.float32)
    return out


def final_norm(residual, lnf_c):
    return layer_norm(residual, lnf_c[0], lnf_c[1]).astype(jnp.bfloat16)


def square_flip(tile):
    fill = jnp.zeros((LANES - tile.shape[0], LANES), jnp.float32)
    return jnp.transpose(jnp.concatenate([tile, fill], axis=0))


def lookup_kernel(ids_ref, blocks_ref, *refs):
    out_refs, (table_ref, rows_ref) = refs[:-2], refs[-2:]
    parts, shard, width = blocks_ref.shape

    def build(j, carry):
        for k in range(width // LANES):
            tile = blocks_ref[j, :, k * LANES:(k + 1) * LANES].astype(jnp.float32)
            table_ref[pl.ds(pl.multiple_of(j * width + k * LANES, LANES), LANES), :] = square_flip(tile)
        return carry

    lax.fori_loop(0, parts, build, 0)
    for which, out_ref in enumerate(out_refs):
        per_part = out_ref.shape[2] // LANES

        def pick(g, carry):
            for v in range(LANES // 8):
                rows = [table_ref[pl.ds(ids_ref[which, g * LANES + v * 8 + u], 1), :] for u in range(8)]
                rows_ref[v * 8:(v + 1) * 8, :] = jnp.concatenate(rows, axis=0)
            flip = jnp.transpose(rows_ref[...])[:shard].astype(jnp.bfloat16)
            out_ref[g // per_part, :, pl.ds(pl.multiple_of(g % per_part * LANES, LANES), LANES)] = flip
            return carry

        lax.fori_loop(0, out_ref.shape[0] * per_part, pick, 0)


def lookup_rows(ids, blocks, tok_dev):
    sets, tokens = ids.shape
    parts, shard, width = blocks.shape
    return pl.pallas_call(
        lookup_kernel,
        out_shape=[jax.ShapeDtypeStruct((parts, shard, tok_dev), jnp.bfloat16)] * sets,
        in_specs=[pl.BlockSpec(memory_space=pltpu.SMEM), pl.BlockSpec(memory_space=pltpu.VMEM)],
        out_specs=[pl.BlockSpec(memory_space=pltpu.VMEM)] * sets,
        scratch_shapes=[pltpu.VMEM((parts * width, LANES), jnp.float32), pltpu.VMEM((LANES, LANES), jnp.float32)],
        compiler_params=pltpu.CompilerParams(vmem_limit_bytes=VMEM_BYTES),
        cost_estimate=pl.CostEstimate(flops=3 * 10 ** 10, bytes_accessed=blocks.size * 2 + sets * tokens * shard * 2, transcendentals=0),
    )(ids, blocks)


def accumulate_kernel(ids_ref, d_ref, low_ref, high_ref, out_ref, sq_ref, acc_ref, rows_ref):
    parts, shard, width = low_ref.shape
    per_part = d_ref.shape[2] // LANES

    def clear(i, carry):
        acc_ref[pl.ds(pl.multiple_of(i * 512, 512), 512), :] = jnp.zeros((512, LANES), jnp.float32)
        return carry

    lax.fori_loop(0, acc_ref.shape[0] // 512, clear, 0)

    def step(g, carry):
        rows_ref[...] = square_flip(d_ref[g // per_part, :, pl.ds(pl.multiple_of(g % per_part * LANES, LANES), LANES)])
        for v in range(LANES // 8):
            rows = rows_ref[v * 8:(v + 1) * 8, :]
            for u in range(8):
                idx = ids_ref[0, g * LANES + v * 8 + u]
                acc_ref[pl.ds(idx, 1), :] = acc_ref[pl.ds(idx, 1), :] + rows[u:u + 1, :]
        return carry

    lax.fori_loop(0, parts * per_part, step, 0)

    def emit(j, total):
        for half, head_ref in enumerate((low_ref, high_ref)):
            for k in range(width // LANES):
                place = pl.ds(pl.multiple_of((2 * j + half) * width + k * LANES, LANES), LANES)
                grad = jnp.transpose(acc_ref[place, :])[:shard] + head_ref[j, :, k * LANES:(k + 1) * LANES]
                out_ref[:, place] = grad
                total = total + grad * grad
        return total

    sq_ref[...] = lax.fori_loop(0, parts, emit, jnp.zeros((shard, LANES), jnp.float32))


def accumulate_rows(ids, d_blocks, head_halves):
    parts, shard, width = head_halves[0].shape
    num_rows = 2 * parts * width
    vmem = pl.BlockSpec(memory_space=pltpu.VMEM)
    return pl.pallas_call(
        accumulate_kernel,
        out_shape=(jax.ShapeDtypeStruct((shard, num_rows), jnp.float32), jax.ShapeDtypeStruct((shard, LANES), jnp.float32)),
        in_specs=[pl.BlockSpec(memory_space=pltpu.SMEM), vmem, vmem, vmem],
        out_specs=(vmem, vmem),
        scratch_shapes=[pltpu.VMEM((num_rows, LANES), jnp.float32), pltpu.VMEM((LANES, LANES), jnp.float32)],
        compiler_params=pltpu.CompilerParams(vmem_limit_bytes=VMEM_BYTES),
        cost_estimate=pl.CostEstimate(flops=5 * 10 ** 10, bytes_accessed=num_rows * shard * 8 + d_blocks.size * 4, transcendentals=0),
    )(ids, d_blocks, *head_halves)


def head_forward_kernel(h_ref, head_ref, mask_ref, u_ref, lse_ref, logit_ref):
    h_tile = h_ref[...]
    slice_len = head_ref.shape[1]
    top = jnp.full((h_tile.shape[0], 1), -jnp.inf, jnp.float32)
    for start in range(0, slice_len, VOCAB_TILE):
        cols = slice(start, start + VOCAB_TILE)
        logits = jnp.dot(h_tile, head_ref[:, cols], preferred_element_type=jnp.float32) + mask_ref[:, cols]
        logit_ref[:, cols] = logits
        top = jnp.maximum(top, jnp.max(logits, axis=-1, keepdims=True))
    total = jnp.zeros_like(top)
    for start in range(0, slice_len, VOCAB_TILE):
        cols = slice(start, start + VOCAB_TILE)
        exp_shift = jnp.exp(logit_ref[:, cols] - top)
        total = total + jnp.sum(exp_shift, axis=-1, keepdims=True)
        part = lax.dot_general(exp_shift.astype(jnp.bfloat16), head_ref[:, cols], (((1,), (1,)), ((), ())), preferred_element_type=jnp.float32)
        if start == 0:
            u_ref[...] = part
        else:
            u_ref[...] += part
    u_ref[...] = u_ref[...] * (1.0 / total)
    lse = top + jnp.log(total)
    lse_ref[...] = jnp.transpose(jnp.broadcast_to(lse, (lse.shape[0], LANES)))[:8]


def head_forward(h_all, head_t, mask):
    tokens, d_model = h_all.shape
    slice_len = head_t.shape[1]
    return pl.pallas_call(
        head_forward_kernel,
        grid=(tokens // TOKEN_TILE,),
        out_shape=(jax.ShapeDtypeStruct((tokens, d_model), jnp.float32), jax.ShapeDtypeStruct((8, tokens), jnp.float32)),
        in_specs=[pl.BlockSpec((TOKEN_TILE, d_model), lambda i: (i, 0)), pl.BlockSpec((d_model, slice_len), lambda i: (0, 0)), pl.BlockSpec((1, slice_len), lambda i: (0, 0))],
        out_specs=(pl.BlockSpec((TOKEN_TILE, d_model), lambda i: (i, 0)), pl.BlockSpec((8, TOKEN_TILE), lambda i: (0, i))),
        scratch_shapes=[pltpu.VMEM((TOKEN_TILE, slice_len), jnp.float32)],
        compiler_params=pltpu.CompilerParams(vmem_limit_bytes=VMEM_BYTES, dimension_semantics=('arbitrary',)),
        cost_estimate=pl.CostEstimate(flops=4 * tokens * d_model * slice_len, bytes_accessed=tokens * d_model * 6 + head_t.size * 2, transcendentals=tokens * slice_len),
    )(h_all, head_t, mask)


def as_column(row):
    return jnp.transpose(jnp.broadcast_to(row, (LANES, row.shape[1])))[:, :1]


def head_grad_kernel(inv_tokens, origin, h_ref, head_ref, mask_ref, lse_ref, tgt_ref, *refs):
    init_ref, grad_ref, flip_ref = refs if len(refs) == 3 else (None,) + refs
    h_tile = h_ref[...]
    width = head_ref.shape[1]
    flip_ref[...] = jnp.transpose(h_tile)
    lse = as_column(lse_ref[...])
    tgt = as_column(tgt_ref[...]).astype(jnp.int32)

    @pl.when(pl.program_id(0) == 0)
    def _():
        grad_ref[...] = jnp.zeros_like(grad_ref) if init_ref is None else init_ref[...]

    for start in range(0, width, GRAD_TILE):
        cols = slice(start, start + GRAD_TILE)
        logits = jnp.dot(h_tile, head_ref[:, cols], preferred_element_type=jnp.float32) + mask_ref[:, cols]
        prob = jnp.exp(logits - lse) * inv_tokens
        is_target = lax.broadcasted_iota(jnp.int32, logits.shape, 1) == tgt - (origin + start)
        d_logits = jnp.where(is_target, prob - inv_tokens, prob).astype(jnp.bfloat16)
        grad_ref[:, cols] += jnp.dot(flip_ref[...], d_logits, preferred_element_type=jnp.float32)


def head_grad(h_all, head_t, mask, lse, tgt, init, inv_tokens, half):
    tokens, d_model = h_all.shape
    slice_len = head_t.shape[1]
    width = slice_len // 2
    whole = pl.BlockSpec((d_model, width), lambda i: (0, 0))
    row = pl.BlockSpec((1, TOKEN_TILE), lambda i: (0, i))
    extra = () if init is None else (init,)
    return pl.pallas_call(
        functools.partial(head_grad_kernel, inv_tokens, half * width),
        grid=(tokens // TOKEN_TILE,),
        out_shape=jax.ShapeDtypeStruct((d_model, width), jnp.float32),
        in_specs=[pl.BlockSpec((TOKEN_TILE, d_model), lambda i: (i, 0)), pl.BlockSpec((d_model, width), lambda i: (0, half)), pl.BlockSpec((1, width), lambda i: (0, half)), row, row] + [whole] * len(extra),
        out_specs=whole,
        scratch_shapes=[pltpu.VMEM((d_model, TOKEN_TILE), jnp.bfloat16)],
        compiler_params=pltpu.CompilerParams(vmem_limit_bytes=VMEM_BYTES, dimension_semantics=('arbitrary',)),
        cost_estimate=pl.CostEstimate(flops=4 * tokens * d_model * width, bytes_accessed=tokens * d_model * 2 + head_t.size * 3, transcendentals=tokens * width),
    )(h_all, head_t, mask, lse, tgt, *extra)


def adam_update(state, grad, decay):
    moment = BETA_ONE * state[1] + (1.0 - BETA_ONE) * grad
    second = BETA_TWO * state[2] + (1.0 - BETA_TWO) * grad * grad
    m_hat = moment / (1.0 - BETA_ONE ** ADAM_STEP)
    v_hat = second / (1.0 - BETA_TWO ** ADAM_STEP)
    master = state[0] * (1.0 - LEARN_RATE * decay) - LEARN_RATE * m_hat / (jnp.sqrt(v_hat) + ADAM_EPS)
    return jnp.stack([master, moment, second])


def solution(mesh):
    n_dev = mesh.shape['dp']
    row_spec = P('dp', None)
    state_specs = (P(None, None, 'dp'), P(None, None, 'dp'), P(None, None, 'dp', None, None, None), P(None, None, None, None, 'dp'), P(None, None, 'dp', None), P(None, None, 'dp', None), P(None, None, 'dp'), P(None, None, 'dp'))

    def gather(local):
        return lax.all_gather(local, 'dp', axis=0, tiled=False)

    def scatter_sum(full):
        return lax.psum_scatter(full, 'dp', scatter_dimension=0, tiled=False)

    def swap(blocks):
        return lax.all_to_all(blocks, 'dp', split_axis=0, concat_axis=0, tiled=False)

    def train_step(token_ids, target_ids, st_wte, st_wpe, st_qkv, st_proj, st_up, st_down, st_vec, st_lnf):
        num_layers, shard = st_qkv.shape[1], st_qkv.shape[2]
        num_heads = st_qkv.shape[4]
        batch_dev, seq_len = token_ids.shape
        vocab_size = st_wte.shape[1]
        pos_rows = st_wpe.shape[1]
        d_model = shard * n_dev
        ff_shard = st_down.shape[2]
        ff_dim = ff_shard * n_dev
        ff_parts = ff_dim // d_model
        vec_shard = st_vec.shape[2]
        tok_dev = batch_dev * seq_len
        tokens = tok_dev * n_dev
        inv_tokens = 1.0 / tokens
        slice_len = -(-vocab_size // (n_dev * VOCAB_TILE)) * VOCAB_TILE
        vocab_pad = slice_len * n_dev
        me = lax.axis_index('dp')

        head_send = jnp.pad(st_wte[0].T.astype(jnp.bfloat16), ((0, 0), (0, vocab_pad - vocab_size)))
        head_send = jnp.swapaxes(head_send.reshape(shard, n_dev, slice_len), 0, 1)
        ids_all = lax.all_gather(jnp.stack([token_ids, target_ids]), 'dp', axis=1, tiled=True).reshape(2, tokens)
        token_send, target_send = lookup_rows(ids_all, head_send, tok_dev)
        token_rows = swap(token_send).reshape(d_model, tok_dev).T.astype(jnp.float32)

        def half_pack(parts):
            return jnp.concatenate([part.astype(jnp.bfloat16) for part in parts], axis=0)

        pos_pack = st_wpe[0, 2:2 + seq_len].T.reshape(-1, d_model)
        pos_count = pos_pack.shape[0]
        small_rows = jnp.concatenate([st_vec[0], jnp.pad(st_lnf[0].reshape(1, -1), ((0, 0), (0, vec_shard - 2 * shard)))], axis=0)
        small_rows = jnp.pad(small_rows, ((0, (-(num_layers + 1 + pos_count)) % 16), (0, d_model - vec_shard)))
        packs = []
        for layer in range(num_layers):
            qkv = st_qkv[0, layer].reshape(shard, 3, d_model)
            parts = [qkv[:, 0], qkv[:, 1], qkv[:, 2], st_proj[0, layer].reshape(d_model, shard).T]
            packs.append(half_pack(parts + ([pos_pack, small_rows] if layer == 0 else [])))
            packs.append(half_pack([st_up[0, layer, :, c * d_model:(c + 1) * d_model] for c in range(ff_parts)] + [st_down[0, layer]]))
        gathered = [gather(pack) for pack in packs]
        attn_rows = 4 * shard
        first = gathered[0]
        pos_c = first[:, attn_rows:attn_rows + pos_count].reshape(d_model, seq_len).T.astype(jnp.float32)
        small_c = first[:, attn_rows + pos_count:attn_rows + pos_count + num_layers + 1, :vec_shard].astype(jnp.float32)
        lnf_c = jnp.swapaxes(small_c[:, num_layers, :2 * shard].reshape(n_dev, 2, shard), 0, 1).reshape(2, d_model)
        group = n_dev // ff_parts

        residual = token_rows.reshape(batch_dev, seq_len, d_model) + pos_c
        attn_backs, feed_backs = [], []
        for layer in range(num_layers):
            vec = small_c[:, layer].reshape(-1, d_model)
            wts = [gathered[2 * layer][:, c * shard:(c + 1) * shard].reshape(d_model, d_model) for c in range(4)]
            residual, back = jax.vjp(functools.partial(attention_half, num_heads=num_heads), residual, *wts, vec[0], vec[1], vec[2], vec[3], vec[5 + ff_parts], vec[6 + ff_parts])
            attn_backs.append(back)
            feed = gathered[2 * layer + 1]
            ups = tuple(feed[:, c * shard:(c + 1) * shard].reshape(d_model, d_model) for c in range(ff_parts))
            downs = tuple(feed[c * group:(c + 1) * group, ff_parts * shard:].reshape(d_model, d_model) for c in range(ff_parts))
            b1s = tuple(vec[4 + c] for c in range(ff_parts))
            residual, back = jax.vjp(feed_half, residual, ups, downs, b1s, vec[4 + ff_parts], vec[7 + ff_parts], vec[8 + ff_parts])
            feed_backs.append(back)
            if layer == 0:
                head_t = swap(head_send)
                residual, head_t = lax.optimization_barrier((residual, head_t))
                head_t = head_t.reshape(d_model, slice_len)
        normed, norm_back = jax.vjp(final_norm, residual, lnf_c)

        vocab_pos = me * slice_len + lax.broadcasted_iota(jnp.int32, (1, slice_len), 1)
        mask = jnp.where(vocab_pos < vocab_size, 0.0, -1e30).astype(jnp.float32)
        tgt_local = (ids_all[1] - me * slice_len).astype(jnp.float32).reshape(n_dev, batch_dev, seq_len)
        h_alls = [gather(normed[row]).reshape(n_dev * seq_len, d_model) for row in range(batch_dev)]
        target_rows = swap(target_send).reshape(d_model, tok_dev).T.astype(jnp.float32).reshape(batch_dev, seq_len, d_model)
        lse_alls, d_sums, loss_part = [], [], 0.0
        for row in range(batch_dev):
            u_part, lse_part = head_forward(h_alls[row], head_t, mask)
            lse_part = lse_part[0].reshape(-1, LANES)
            lse_dev = gather(lse_part)
            top = jnp.max(lse_dev, axis=0)
            lse = top + jnp.log(jnp.sum(jnp.exp(lse_dev - top), axis=0))
            factor = (jnp.exp(lse_part - lse) * inv_tokens).reshape(n_dev, seq_len, 1)
            scaled = u_part.reshape(n_dev, seq_len, d_model) * factor
            if row + 1 < batch_dev:
                scaled, h_alls[row + 1] = lax.optimization_barrier((scaled, h_alls[row + 1]))
            d_sums.append(scatter_sum(scaled))
            lse_alls.append(lse.reshape(1, -1))
            own = lax.dynamic_slice_in_dim(lse.reshape(n_dev, seq_len), me, 1, axis=0)
            picked = jnp.sum(normed[row].astype(jnp.float32) * target_rows[row], axis=-1)
            loss_part = loss_part + (jnp.sum(own) - jnp.sum(picked)) * inv_tokens
        grad_heads = []
        for half in range(2):
            part = None
            for row in range(batch_dev):
                part = head_grad(h_alls[row], head_t, mask, lse_alls[row], tgt_local[:, row].reshape(1, -1), part, inv_tokens, half)
            grad_heads.append(part.reshape(n_dev, shard, slice_len // 2))
        grad_heads[0] = swap(grad_heads[0])
        d_sums, grad_heads = lax.optimization_barrier((d_sums, grad_heads))
        grad_heads[1] = swap(grad_heads[1])
        d_normed = jnp.stack(d_sums) - inv_tokens * target_rows

        d_resid, d_lnf = norm_back(d_normed.astype(jnp.bfloat16))
        vec_rows = [None] * num_layers
        qkv_g, proj_g, up_g, down_g = ([None] * num_layers for _ in range(4))
        feed_rows = attn_rows + ff_parts * shard
        for layer in reversed(range(num_layers)):
            d_resid, d_ups, d_downs, d_b1s, d_b2, d_gain2, d_shift2 = feed_backs[layer](d_resid)
            if layer == num_layers - 1:
                d_resid, grad_heads = lax.optimization_barrier((d_resid, grad_heads))
            d_resid, d_q, d_k, d_v, d_proj, d_bq, d_bk, d_bv, d_bo, d_gain1, d_shift1 = attn_backs[layer](d_resid)
            vec_rows[layer] = jnp.stack([d_bq, d_bk, d_bv, d_bo, *d_b1s, d_b2, d_gain1, d_shift1, d_gain2, d_shift2]).reshape(n_dev, 1, vec_shard)
            parts = [g.reshape(n_dev, shard, d_model) for g in (d_q, d_k, d_v, d_proj, *d_ups)]
            parts.append(jnp.concatenate([g.reshape(group, ff_shard, d_model) for g in d_downs], axis=0))
            parts = [part.astype(jnp.float32) for part in parts]
            if layer == 0:
                pos_sum = jnp.sum(d_resid, axis=0).T.reshape(n_dev, pos_count, d_model)
                rows = jnp.pad(jnp.swapaxes(d_lnf.reshape(2, n_dev, shard), 0, 1).reshape(n_dev, 1, 2 * shard), ((0, 0), (0, 0), (0, vec_shard - 2 * shard)))
                rows = jnp.concatenate(vec_rows + [rows], axis=1)
                rows = jnp.pad(rows, ((0, 0), (0, (-(num_layers + 1 + pos_count)) % 8), (0, d_model - vec_shard)))
                parts = parts + [pos_sum, rows]
            summed = scatter_sum(jnp.concatenate(parts, axis=1))
            qkv_g[layer] = jnp.swapaxes(summed[:3 * shard].reshape(3, shard, d_model), 0, 1).reshape(st_qkv.shape[2:])
            proj_g[layer] = summed[3 * shard:attn_rows].T.reshape(st_proj.shape[2:])
            up_g[layer] = jnp.swapaxes(summed[attn_rows:feed_rows].reshape(ff_parts, shard, d_model), 0, 1).reshape(shard, ff_dim)
            down_g[layer] = summed[feed_rows:feed_rows + ff_shard]
            if layer == 0:
                tail = feed_rows + ff_shard
                pos_g = jnp.pad(summed[tail:tail + pos_count].reshape(shard, seq_len).T, ((2, pos_rows - 2 - seq_len), (0, 0)))
                small_g = summed[tail + pos_count:tail + pos_count + num_layers + 1, :vec_shard]
        vec_g = small_g[:num_layers]
        lnf_g = small_g[num_layers, :2 * shard].reshape(2, shard)

        lookup_d = swap(d_resid.reshape(tok_dev, d_model).T.reshape(n_dev, shard, tok_dev))
        wte_g, wte_sq = accumulate_rows(ids_all, lookup_d, grad_heads)

        grads = [pos_g, jnp.stack(qkv_g), jnp.stack(proj_g), jnp.stack(up_g), jnp.stack(down_g), vec_g, lnf_g]
        local_sq = jnp.sum(wte_sq) + sum(jnp.sum(grad * grad) for grad in grads)
        sums = lax.psum(jnp.stack([local_sq, loss_part]), 'dp')
        clip_coef = jnp.minimum(1.0, CLIP_NORM / (jnp.sqrt(sums[0]) + 1e-6))
        new_wte = jnp.swapaxes(adam_update(jnp.swapaxes(st_wte, 1, 2), wte_g[:, :vocab_size] * clip_coef, DECAYS[0]), 1, 2)
        states = (st_wpe, st_qkv, st_proj, st_up, st_down, st_vec, st_lnf)
        new_states = tuple(adam_update(state, grad * clip_coef, decay) for state, grad, decay in zip(states, grads, DECAYS[1:]))
        return (sums[1], new_wte) + new_states

    return jax.shard_map(train_step, mesh=mesh, in_specs=(row_spec, row_spec) + state_specs, out_specs=(P(),) + state_specs, check_vma=False)
```

```python
import functools

import jax
import jax.numpy as jnp
from jax import lax
from jax.experimental import pallas as pl
from jax.experimental.pallas import tpu as pltpu
from jax.sharding import PartitionSpec as P

NORM_EPS = 1e-5
LEARN_RATE = 3e-3
BETA_ONE = 0.9
BETA_TWO = 0.95
ADAM_EPS = 1e-8
WEIGHT_DECAY = 0.1
CLIP_NORM = 1.0
ADAM_STEP = 10
DECAYS = (WEIGHT_DECAY,) * 6 + (0.0, 0.0)
LANES = 128
TOKEN_TILE = 512
VOCAB_TILE = 512
GRAD_TILE = 640
GRAD_TOKENS = 1024
VMEM_BYTES = 60 * 1024 * 1024


def layer_norm(residual, gain, bias):
    mean_val = jnp.mean(residual, axis=-1, keepdims=True)
    centered = residual - mean_val
    variance = jnp.mean(centered * centered, axis=-1, keepdims=True)
    return centered * lax.rsqrt(variance + NORM_EPS) * gain.astype(jnp.float32) + bias.astype(jnp.float32)


def affine(x, weight, bias):
    return jnp.einsum('bsd,de->bse', x, weight, preferred_element_type=jnp.float32) + bias


def attention_half(residual, wq, wk, wv, proj_t, bq, bk, bv, bo, gain, shift, num_heads):
    batch, seq_len, d_model = residual.shape
    head_dim = d_model // num_heads
    normed_in = layer_norm(residual, gain, shift).astype(jnp.bfloat16)
    q, k, v = (affine(normed_in, w, b).astype(jnp.bfloat16).reshape(batch, seq_len, num_heads, head_dim) for w, b in ((wq, bq), (wk, bk), (wv, bv)))
    scores = jnp.einsum('bqhk,bshk->bhqs', q, k, preferred_element_type=jnp.float32) * head_dim ** -0.5
    rows_iota = lax.broadcasted_iota(jnp.int32, (seq_len, seq_len), 0)
    cols_iota = lax.broadcasted_iota(jnp.int32, (seq_len, seq_len), 1)
    scores = jnp.where(rows_iota >= cols_iota, scores, -1e30)
    attn_prob = jax.nn.softmax(scores, axis=-1).astype(jnp.bfloat16)
    mixed = jnp.einsum('bhqs,bshk->bqhk', attn_prob, v, preferred_element_type=jnp.float32).astype(jnp.bfloat16)
    mixed = mixed.reshape(batch, seq_len, d_model)
    return residual + jnp.einsum('bsl,el->bse', mixed, proj_t, preferred_element_type=jnp.float32) + bo


def feed_half(residual, ups, downs, b1s, b2, gain, shift):
    normed_mid = layer_norm(residual, gain, shift).astype(jnp.bfloat16)
    out = residual + b2
    for up_w, down_w, b1 in zip(ups, downs, b1s):
        hidden = jax.nn.relu(affine(normed_mid, up_w, b1)).astype(jnp.bfloat16)
        out = out + jnp.einsum('bsf,fd->bsd', hidden, down_w, preferred_element_type=jnp.float32)
    return out


def final_norm(residual, lnf_c):
    return layer_norm(residual, lnf_c[0], lnf_c[1]).astype(jnp.bfloat16)


def square_flip(tile):
    fill = jnp.zeros((LANES - tile.shape[0], LANES), jnp.float32)
    return jnp.transpose(jnp.concatenate([tile, fill], axis=0))


def lookup_kernel(ids_ref, blocks_ref, *refs):
    out_refs, (table_ref, rows_ref) = refs[:-2], refs[-2:]
    parts, shard, width = blocks_ref.shape

    def build(j, carry):
        for k in range(width // LANES):
            tile = blocks_ref[j, :, k * LANES:(k + 1) * LANES].astype(jnp.float32)
            table_ref[pl.ds(pl.multiple_of(j * width + k * LANES, LANES), LANES), :] = square_flip(tile)
        return carry

    lax.fori_loop(0, parts, build, 0)
    for which, out_ref in enumerate(out_refs):
        per_part = out_ref.shape[2] // LANES

        def pick(g, carry):
            for v in range(LANES // 8):
                rows = [table_ref[pl.ds(ids_ref[which, g * LANES + v * 8 + u], 1), :] for u in range(8)]
                rows_ref[v * 8:(v + 1) * 8, :] = jnp.concatenate(rows, axis=0)
            flip = jnp.transpose(rows_ref[...])[:shard].astype(jnp.bfloat16)
            out_ref[g // per_part, :, pl.ds(pl.multiple_of(g % per_part * LANES, LANES), LANES)] = flip
            return carry

        lax.fori_loop(0, out_ref.shape[0] * per_part, pick, 0)


def lookup_rows(ids, blocks, tok_dev):
    sets, tokens = ids.shape
    parts, shard, width = blocks.shape
    return pl.pallas_call(
        lookup_kernel,
        out_shape=[jax.ShapeDtypeStruct((parts, shard, tok_dev), jnp.bfloat16)] * sets,
        in_specs=[pl.BlockSpec(memory_space=pltpu.SMEM), pl.BlockSpec(memory_space=pltpu.VMEM)],
        out_specs=[pl.BlockSpec(memory_space=pltpu.VMEM)] * sets,
        scratch_shapes=[pltpu.VMEM((parts * width, LANES), jnp.float32), pltpu.VMEM((LANES, LANES), jnp.float32)],
        compiler_params=pltpu.CompilerParams(vmem_limit_bytes=VMEM_BYTES),
        cost_estimate=pl.CostEstimate(flops=3 * 10 ** 10, bytes_accessed=blocks.size * 2 + sets * tokens * shard * 2, transcendentals=0),
    )(ids, blocks)


def accumulate_kernel(ids_ref, d_ref, low_ref, high_ref, out_ref, sq_ref, acc_ref, rows_ref):
    parts, shard, width = low_ref.shape
    per_part = d_ref.shape[2] // LANES

    def clear(i, carry):
        acc_ref[pl.ds(pl.multiple_of(i * 512, 512), 512), :] = jnp.zeros((512, LANES), jnp.float32)
        return carry

    lax.fori_loop(0, acc_ref.shape[0] // 512, clear, 0)

    def step(g, carry):
        rows_ref[...] = square_flip(d_ref[g // per_part, :, pl.ds(pl.multiple_of(g % per_part * LANES, LANES), LANES)])
        for v in range(LANES // 8):
            rows = rows_ref[v * 8:(v + 1) * 8, :]
            for u in range(8):
                idx = ids_ref[0, g * LANES + v * 8 + u]
                acc_ref[pl.ds(idx, 1), :] = acc_ref[pl.ds(idx, 1), :] + rows[u:u + 1, :]
        return carry

    lax.fori_loop(0, parts * per_part, step, 0)

    def emit(j, total):
        for half, head_ref in enumerate((low_ref, high_ref)):
            for k in range(width // LANES):
                place = pl.ds(pl.multiple_of((2 * j + half) * width + k * LANES, LANES), LANES)
                grad = jnp.transpose(acc_ref[place, :])[:shard] + head_ref[j, :, k * LANES:(k + 1) * LANES]
                out_ref[:, place] = grad
                total = total + grad * grad
        return total

    sq_ref[...] = lax.fori_loop(0, parts, emit, jnp.zeros((shard, LANES), jnp.float32))


def accumulate_rows(ids, d_blocks, head_halves):
    parts, shard, width = head_halves[0].shape
    num_rows = 2 * parts * width
    vmem = pl.BlockSpec(memory_space=pltpu.VMEM)
    return pl.pallas_call(
        accumulate_kernel,
        out_shape=(jax.ShapeDtypeStruct((shard, num_rows), jnp.float32), jax.ShapeDtypeStruct((shard, LANES), jnp.float32)),
        in_specs=[pl.BlockSpec(memory_space=pltpu.SMEM), vmem, vmem, vmem],
        out_specs=(vmem, vmem),
        scratch_shapes=[pltpu.VMEM((num_rows, LANES), jnp.float32), pltpu.VMEM((LANES, LANES), jnp.float32)],
        compiler_params=pltpu.CompilerParams(vmem_limit_bytes=VMEM_BYTES),
        cost_estimate=pl.CostEstimate(flops=5 * 10 ** 10, bytes_accessed=num_rows * shard * 8 + d_blocks.size * 4, transcendentals=0),
    )(ids, d_blocks, *head_halves)


def head_forward_kernel(h_ref, head_ref, mask_ref, u_ref, lse_ref, logit_ref):
    h_tile = h_ref[...]
    slice_len = head_ref.shape[1]
    top = jnp.full((h_tile.shape[0], 1), -jnp.inf, jnp.float32)
    for start in range(0, slice_len, VOCAB_TILE):
        cols = slice(start, start + VOCAB_TILE)
        logits = jnp.dot(h_tile, head_ref[:, cols], preferred_element_type=jnp.float32) + mask_ref[:, cols]
        logit_ref[:, cols] = logits
        top = jnp.maximum(top, jnp.max(logits, axis=-1, keepdims=True))
    total = jnp.zeros_like(top)
    for start in range(0, slice_len, VOCAB_TILE):
        cols = slice(start, start + VOCAB_TILE)
        exp_shift = jnp.exp(logit_ref[:, cols] - top)
        total = total + jnp.sum(exp_shift, axis=-1, keepdims=True)
        part = lax.dot_general(exp_shift.astype(jnp.bfloat16), head_ref[:, cols], (((1,), (1,)), ((), ())), preferred_element_type=jnp.float32)
        if start == 0:
            u_ref[...] = part
        else:
            u_ref[...] += part
    u_ref[...] = u_ref[...] * (1.0 / total)
    lse = top + jnp.log(total)
    lse_ref[...] = jnp.transpose(jnp.broadcast_to(lse, (lse.shape[0], LANES)))[:8]


def head_forward(h_all, head_t, mask):
    tokens, d_model = h_all.shape
    slice_len = head_t.shape[1]
    return pl.pallas_call(
        head_forward_kernel,
        grid=(tokens // TOKEN_TILE,),
        out_shape=(jax.ShapeDtypeStruct((tokens, d_model), jnp.float32), jax.ShapeDtypeStruct((8, tokens), jnp.float32)),
        in_specs=[pl.BlockSpec((TOKEN_TILE, d_model), lambda i: (i, 0)), pl.BlockSpec((d_model, slice_len), lambda i: (0, 0)), pl.BlockSpec((1, slice_len), lambda i: (0, 0))],
        out_specs=(pl.BlockSpec((TOKEN_TILE, d_model), lambda i: (i, 0)), pl.BlockSpec((8, TOKEN_TILE), lambda i: (0, i))),
        scratch_shapes=[pltpu.VMEM((TOKEN_TILE, slice_len), jnp.float32)],
        compiler_params=pltpu.CompilerParams(vmem_limit_bytes=VMEM_BYTES, dimension_semantics=('arbitrary',)),
        cost_estimate=pl.CostEstimate(flops=4 * tokens * d_model * slice_len, bytes_accessed=tokens * d_model * 6 + head_t.size * 2, transcendentals=tokens * slice_len),
    )(h_all, head_t, mask)


def as_column(row):
    return jnp.transpose(jnp.broadcast_to(row, (LANES, row.shape[1])))[:, :1]


def head_grad_kernel(inv_tokens, origin, h_ref, head_ref, mask_ref, lse_ref, tgt_ref, *refs):
    init_ref, grad_ref, flip_ref = refs if len(refs) == 3 else (None,) + refs
    h_tile = h_ref[...]
    width = head_ref.shape[1]
    flip_ref[...] = jnp.transpose(h_tile)
    lse = as_column(lse_ref[...])
    tgt = as_column(tgt_ref[...]).astype(jnp.int32)

    @pl.when(pl.program_id(0) == 0)
    def _():
        grad_ref[...] = jnp.zeros_like(grad_ref) if init_ref is None else init_ref[...]

    for start in range(0, width, GRAD_TILE):
        cols = slice(start, start + GRAD_TILE)
        logits = jnp.dot(h_tile, head_ref[:, cols], preferred_element_type=jnp.float32) + mask_ref[:, cols]
        prob = jnp.exp(logits - lse) * inv_tokens
        is_target = lax.broadcasted_iota(jnp.int32, logits.shape, 1) == tgt - (origin + start)
        d_logits = jnp.where(is_target, prob - inv_tokens, prob).astype(jnp.bfloat16)
        grad_ref[:, cols] += jnp.dot(flip_ref[...], d_logits, preferred_element_type=jnp.float32)


def head_grad(h_all, head_t, mask, lse, tgt, init, inv_tokens, half):
    tokens, d_model = h_all.shape
    slice_len = head_t.shape[1]
    width = slice_len // 2
    whole = pl.BlockSpec((d_model, width), lambda i: (0, 0))
    row = pl.BlockSpec((1, GRAD_TOKENS), lambda i: (0, i))
    extra = () if init is None else (init,)
    return pl.pallas_call(
        functools.partial(head_grad_kernel, inv_tokens, half * width),
        grid=(tokens // GRAD_TOKENS,),
        out_shape=jax.ShapeDtypeStruct((d_model, width), jnp.float32),
        in_specs=[pl.BlockSpec((GRAD_TOKENS, d_model), lambda i: (i, 0)), pl.BlockSpec((d_model, width), lambda i: (0, half)), pl.BlockSpec((1, width), lambda i: (0, half)), row, row] + [whole] * len(extra),
        out_specs=whole,
        scratch_shapes=[pltpu.VMEM((d_model, GRAD_TOKENS), jnp.bfloat16)],
        compiler_params=pltpu.CompilerParams(vmem_limit_bytes=VMEM_BYTES, dimension_semantics=('arbitrary',)),
        cost_estimate=pl.CostEstimate(flops=4 * tokens * d_model * width, bytes_accessed=tokens * d_model * 2 + head_t.size * 3, transcendentals=tokens * width),
    )(h_all, head_t, mask, lse, tgt, *extra)


def adam_update(state, grad, decay):
    moment = BETA_ONE * state[1] + (1.0 - BETA_ONE) * grad
    second = BETA_TWO * state[2] + (1.0 - BETA_TWO) * grad * grad
    m_hat = moment / (1.0 - BETA_ONE ** ADAM_STEP)
    v_hat = second / (1.0 - BETA_TWO ** ADAM_STEP)
    master = state[0] * (1.0 - LEARN_RATE * decay) - LEARN_RATE * m_hat / (jnp.sqrt(v_hat) + ADAM_EPS)
    return jnp.stack([master, moment, second])


def solution(mesh):
    n_dev = mesh.shape['dp']
    row_spec = P('dp', None)
    state_specs = (P(None, None, 'dp'), P(None, None, 'dp'), P(None, None, 'dp', None, None, None), P(None, None, None, None, 'dp'), P(None, None, 'dp', None), P(None, None, 'dp', None), P(None, None, 'dp'), P(None, None, 'dp'))

    def gather(local):
        return lax.all_gather(local, 'dp', axis=0, tiled=False)

    def scatter_sum(full):
        return lax.psum_scatter(full, 'dp', scatter_dimension=0, tiled=False)

    def swap(blocks):
        return lax.all_to_all(blocks, 'dp', split_axis=0, concat_axis=0, tiled=False)

    def train_step(token_ids, target_ids, st_wte, st_wpe, st_qkv, st_proj, st_up, st_down, st_vec, st_lnf):
        num_layers, shard = st_qkv.shape[1], st_qkv.shape[2]
        num_heads = st_qkv.shape[4]
        batch_dev, seq_len = token_ids.shape
        vocab_size = st_wte.shape[1]
        pos_rows = st_wpe.shape[1]
        d_model = shard * n_dev
        ff_shard = st_down.shape[2]
        ff_dim = ff_shard * n_dev
        ff_parts = ff_dim // d_model
        vec_shard = st_vec.shape[2]
        tok_dev = batch_dev * seq_len
        tokens = tok_dev * n_dev
        inv_tokens = 1.0 / tokens
        slice_len = -(-vocab_size // (n_dev * VOCAB_TILE)) * VOCAB_TILE
        vocab_pad = slice_len * n_dev
        me = lax.axis_index('dp')

        head_send = jnp.pad(st_wte[0].T.astype(jnp.bfloat16), ((0, 0), (0, vocab_pad - vocab_size)))
        head_send = jnp.swapaxes(head_send.reshape(shard, n_dev, slice_len), 0, 1)
        ids_all = lax.all_gather(jnp.stack([token_ids, target_ids]), 'dp', axis=1, tiled=True).reshape(2, tokens)
        token_send, = lookup_rows(ids_all[:1], head_send, tok_dev)
        token_rows = swap(token_send).reshape(d_model, tok_dev).T.astype(jnp.float32)

        def half_pack(parts):
            return jnp.concatenate([part.astype(jnp.bfloat16) for part in parts], axis=0)

        pos_pack = st_wpe[0, 2:2 + seq_len].T.reshape(-1, d_model)
        pos_count = pos_pack.shape[0]
        small_rows = jnp.concatenate([st_vec[0], jnp.pad(st_lnf[0].reshape(1, -1), ((0, 0), (0, vec_shard - 2 * shard)))], axis=0)
        small_rows = jnp.pad(small_rows, ((0, (-(num_layers + 1 + pos_count)) % 16), (0, d_model - vec_shard)))
        packs = []
        for layer in range(num_layers):
            qkv = st_qkv[0, layer].reshape(shard, 3, d_model)
            parts = [qkv[:, 0], qkv[:, 1], qkv[:, 2], st_proj[0, layer].reshape(d_model, shard).T]
            packs.append(half_pack(parts + ([pos_pack, small_rows] if layer == 0 else [])))
            packs.append(half_pack([st_up[0, layer, :, c * d_model:(c + 1) * d_model] for c in range(ff_parts)] + [st_down[0, layer]]))
        gathered = [gather(pack) for pack in packs]
        attn_rows = 4 * shard
        first = gathered[0]
        pos_c = first[:, attn_rows:attn_rows + pos_count].reshape(d_model, seq_len).T.astype(jnp.float32)
        small_c = first[:, attn_rows + pos_count:attn_rows + pos_count + num_layers + 1, :vec_shard].astype(jnp.float32)
        lnf_c = jnp.swapaxes(small_c[:, num_layers, :2 * shard].reshape(n_dev, 2, shard), 0, 1).reshape(2, d_model)
        group = n_dev // ff_parts

        residual = token_rows.reshape(batch_dev, seq_len, d_model) + pos_c
        attn_backs, feed_backs = [], []
        for layer in range(num_layers):
            vec = small_c[:, layer].reshape(-1, d_model)
            wts = [gathered[2 * layer][:, c * shard:(c + 1) * shard].reshape(d_model, d_model) for c in range(4)]
            residual, back = jax.vjp(functools.partial(attention_half, num_heads=num_heads), residual, *wts, vec[0], vec[1], vec[2], vec[3], vec[5 + ff_parts], vec[6 + ff_parts])
            attn_backs.append(back)
            feed = gathered[2 * layer + 1]
            ups = tuple(feed[:, c * shard:(c + 1) * shard].reshape(d_model, d_model) for c in range(ff_parts))
            downs = tuple(feed[c * group:(c + 1) * group, ff_parts * shard:].reshape(d_model, d_model) for c in range(ff_parts))
            b1s = tuple(vec[4 + c] for c in range(ff_parts))
            residual, back = jax.vjp(feed_half, residual, ups, downs, b1s, vec[4 + ff_parts], vec[7 + ff_parts], vec[8 + ff_parts])
            feed_backs.append(back)
            if layer == 0:
                head_t = swap(head_send)
                residual, head_t = lax.optimization_barrier((residual, head_t))
                head_t = head_t.reshape(d_model, slice_len)
        normed, norm_back = jax.vjp(final_norm, residual, lnf_c)

        vocab_pos = me * slice_len + lax.broadcasted_iota(jnp.int32, (1, slice_len), 1)
        mask = jnp.where(vocab_pos < vocab_size, 0.0, -1e30).astype(jnp.float32)
        tgt_local = (ids_all[1] - me * slice_len).astype(jnp.float32).reshape(n_dev, batch_dev, seq_len)
        h_alls = [gather(normed[row]).reshape(n_dev * seq_len, d_model) for row in range(batch_dev)]
        late_ids, _ = lax.optimization_barrier((ids_all[1:], normed))
        target_send, = lookup_rows(late_ids, head_send, tok_dev)
        head_t, target_send = lax.optimization_barrier((head_t, target_send))
        target_rows = swap(target_send).reshape(d_model, tok_dev).T.astype(jnp.float32).reshape(batch_dev, seq_len, d_model)
        lse_alls, d_sums, loss_part = [], [], 0.0
        for row in range(batch_dev):
            u_part, lse_part = head_forward(h_alls[row], head_t, mask)
            lse_part = lse_part[0].reshape(-1, LANES)
            lse_dev = gather(lse_part)
            top = jnp.max(lse_dev, axis=0)
            lse = top + jnp.log(jnp.sum(jnp.exp(lse_dev - top), axis=0))
            factor = (jnp.exp(lse_part - lse) * inv_tokens).reshape(n_dev, seq_len, 1)
            scaled = u_part.reshape(n_dev, seq_len, d_model) * factor
            if row + 1 < batch_dev:
                scaled, h_alls[row + 1] = lax.optimization_barrier((scaled, h_alls[row + 1]))
            d_sums.append(scatter_sum(scaled))
            lse_alls.append(lse.reshape(1, -1))
            own = lax.dynamic_slice_in_dim(lse.reshape(n_dev, seq_len), me, 1, axis=0)
            picked = jnp.sum(normed[row].astype(jnp.float32) * target_rows[row], axis=-1)
            loss_part = loss_part + (jnp.sum(own) - jnp.sum(picked)) * inv_tokens
        grad_heads = []
        for half in range(2):
            part = None
            for row in range(batch_dev):
                part = head_grad(h_alls[row], head_t, mask, lse_alls[row], tgt_local[:, row].reshape(1, -1), part, inv_tokens, half)
            grad_heads.append(part.reshape(n_dev, shard, slice_len // 2))
        grad_heads[0] = swap(grad_heads[0])
        d_sums, grad_heads = lax.optimization_barrier((d_sums, grad_heads))
        grad_heads[1] = swap(grad_heads[1])
        d_normed = jnp.stack(d_sums) - inv_tokens * target_rows

        d_resid, d_lnf = norm_back(d_normed.astype(jnp.bfloat16))
        vec_rows, packed_sums = [None] * num_layers, []
        qkv_g, proj_g, up_g, down_g = ([None] * num_layers for _ in range(4))
        feed_rows = attn_rows + ff_parts * shard
        for layer in reversed(range(num_layers)):
            d_resid, d_ups, d_downs, d_b1s, d_b2, d_gain2, d_shift2 = feed_backs[layer](d_resid)
            if layer == num_layers - 1:
                d_resid, grad_heads = lax.optimization_barrier((d_resid, grad_heads))
            d_resid, d_q, d_k, d_v, d_proj, d_bq, d_bk, d_bv, d_bo, d_gain1, d_shift1 = attn_backs[layer](d_resid)
            vec_rows[layer] = jnp.stack([d_bq, d_bk, d_bv, d_bo, *d_b1s, d_b2, d_gain1, d_shift1, d_gain2, d_shift2]).reshape(n_dev, 1, vec_shard)
            parts = [g.reshape(n_dev, shard, d_model) for g in (d_q, d_k, d_v, d_proj, *d_ups)]
            parts.append(jnp.concatenate([g.reshape(group, ff_shard, d_model) for g in d_downs], axis=0))
            parts = [part.astype(jnp.float32) for part in parts]
            if layer == 0:
                pos_sum = jnp.sum(d_resid, axis=0).T.reshape(n_dev, pos_count, d_model)
                rows = jnp.pad(jnp.swapaxes(d_lnf.reshape(2, n_dev, shard), 0, 1).reshape(n_dev, 1, 2 * shard), ((0, 0), (0, 0), (0, vec_shard - 2 * shard)))
                rows = jnp.concatenate(vec_rows + [rows], axis=1)
                rows = jnp.pad(rows, ((0, 0), (0, (-(num_layers + 1 + pos_count)) % 8), (0, d_model - vec_shard)))
                parts = parts + [pos_sum, rows]
            summed = scatter_sum(jnp.concatenate(parts, axis=1))
            packed_sums.append(summed)
            qkv_g[layer] = jnp.swapaxes(summed[:3 * shard].reshape(3, shard, d_model), 0, 1).reshape(st_qkv.shape[2:])
            proj_g[layer] = summed[3 * shard:attn_rows].T.reshape(st_proj.shape[2:])
            up_g[layer] = jnp.swapaxes(summed[attn_rows:feed_rows].reshape(ff_parts, shard, d_model), 0, 1).reshape(shard, ff_dim)
            down_g[layer] = summed[feed_rows:feed_rows + ff_shard]
            if layer == 0:
                tail = feed_rows + ff_shard
                pos_g = jnp.pad(summed[tail:tail + pos_count].reshape(shard, seq_len).T, ((2, pos_rows - 2 - seq_len), (0, 0)))
                small_g = summed[tail + pos_count:tail + pos_count + num_layers + 1, :vec_shard]
        vec_g = small_g[:num_layers]
        lnf_g = small_g[num_layers, :2 * shard].reshape(2, shard)

        lookup_d = swap(d_resid.reshape(tok_dev, d_model).T.reshape(n_dev, shard, tok_dev))
        wte_g, wte_sq = accumulate_rows(ids_all, lookup_d, grad_heads)

        local_sq = jnp.sum(wte_sq) + sum(jnp.sum(summed * summed) for summed in packed_sums)
        grads = [pos_g, jnp.stack(qkv_g), jnp.stack(proj_g), jnp.stack(up_g), jnp.stack(down_g), vec_g, lnf_g]
        sums = jnp.sum(gather(jnp.pad(jnp.stack([local_sq, loss_part]), (0, LANES - 2))), axis=0)
        clip_coef = jnp.minimum(1.0, CLIP_NORM / (jnp.sqrt(sums[0]) + 1e-6))
        new_wte = jnp.swapaxes(adam_update(jnp.swapaxes(st_wte, 1, 2), wte_g[:, :vocab_size] * clip_coef, DECAYS[0]), 1, 2)
        states = (st_wpe, st_qkv, st_proj, st_up, st_down, st_vec, st_lnf)
        new_states = tuple(adam_update(state, grad * clip_coef, decay) for state, grad, decay in zip(states, grads, DECAYS[1:]))
        return (sums[1], new_wte) + new_states

    return jax.shard_map(train_step, mesh=mesh, in_specs=(row_spec, row_spec) + state_specs, out_specs=(P(),) + state_specs, check_vma=False)
```
